32 devices in a mesh: section: 4 (over y, x), fsdp: 8 (over z, core).
Axes of the slice: x: 2, y: 2, z: 4, core: 2. Of those that a mesh axis runs over, the one named last changes fastest.
Arguments:
- grad_parts: bfloat16 [4, 8, 8192, 1024], P('section', 'fsdp'), may hold values from -510 to 510
- first_codes: int32 [4, 8192, 1024], P('section', 'fsdp'), may hold values from -7 to 7
- first_rows: float32 [4, 8192], P('section', 'fsdp'), may hold values from 0.003 to 0.03
- first_columns: float32 [4, 1024], P('section'), may hold values from 0.003 to 0.03
- second_codes: int32 [4, 8192, 1024], P('section', 'fsdp'), may hold values from 1 to 15
- second_rows: float32 [4, 8192], P('section', 'fsdp'), may hold values from 0.001 to 0.01
- second_columns: float32 [4, 1024], P('section'), may hold values from 0.001 to 0.01
Outputs:
- direction: float32 [4, 8192, 1024], P('section', 'fsdp')
- first_scaled: float32 [4, 8192, 1024], P('section', 'fsdp')
- second_scaled: float32 [4, 8192, 1024], P('section', 'fsdp')
- first_rowmax: float32 [4, 8192], P('section', 'fsdp')
- first_colmax: float32 [4, 1024], P('section')
- second_rowmax: float32 [4, 8192], P('section', 'fsdp')
- second_colmax: float32 [4, 1024], P('section')
The draws below stay inside these ranges and needn't reach their ends.
All inputs are finite; a program needn't handle non-finite values. Where the reference program divides by a largest or mean magnitude, that divisor is 1e-20 or more.
Results may differ from the reference program's by a relative error of at most 0.0003.
Values may be sent and summed in bfloat16 or wider, within the bound.
A program may use at most 192 MiB of HBM per device.

```python
import math
import jax
import jax.numpy as jnp
from jax import lax

ROWS = 8192
KV = 1024
LAYERS_ALL = 4
PARTIALS = 8


def draw_grad_parts(key, part):
    subkeys = jax.random.split(key, 5)
    full_shape = (LAYERS_ALL, PARTIALS, ROWS, KV)
    col_scale = jnp.exp(jax.random.uniform(subkeys[0], (LAYERS_ALL, 1, 1, KV), jnp.float32, math.log(0.2), math.log(5.0)))
    row_scale = jnp.exp(jax.random.uniform(subkeys[1], (LAYERS_ALL, 1, ROWS, 1), jnp.float32, math.log(0.5), math.log(2.0)))
    owner_block = jax.random.randint(subkeys[2], (LAYERS_ALL, PARTIALS, 1, 1), 0, PARTIALS)
    row_block = (jnp.arange(ROWS, dtype=jnp.int32) // (ROWS // PARTIALS)).reshape(1, 1, ROWS, 1)
    spike_gain = jnp.where(row_block == owner_block, 4.0, 1.0)
    basis_values = jnp.clip(jax.random.normal(subkeys[3], full_shape, jnp.float32), -6.0, 6.0)
    return (basis_values * col_scale * row_scale * spike_gain).astype(jnp.bfloat16)


def plant(result, key, least, high):
    longest = result.shape.index(max(result.shape))
    spots = []
    for shift in (0, 1):
        where = [jax.random.randint(jax.random.fold_in(key, axis), (), 0, length) for axis, length in enumerate(result.shape)]
        where[longest] = (where[longest] + shift) % result.shape[longest]
        spots.append(tuple(where))
    return result.at[spots[0]].set(least).at[spots[1]].set(high)


def shard_levels(rng, extent, cuts, least, largest):
    factor_of = 1.0
    for position, shards_of in cuts:
        heights = jax.random.uniform(jax.random.fold_in(jax.random.fold_in(rng, 6), position), (shards_of,), jnp.float32, least / len(cuts), largest / len(cuts))
        factor_of = factor_of * jnp.repeat(jnp.exp(heights), extent[position] // shards_of).reshape((-1,) + (1,) * (len(extent) - 1 - position))
    return factor_of


def setup_inputs(seed: int = 0) -> dict:
    keys = jax.random.split(jax.random.key(seed), 8)
    return {
        "grad_parts": draw_grad_parts(jax.random.fold_in(keys[7], 71), 0),
        "first_codes": plant(jax.random.randint(keys[1], (LAYERS_ALL, ROWS, KV), -7, 8), jax.random.fold_in(keys[1], 1), -7, 7).astype(jnp.int32),
        "first_rows": jnp.clip(jnp.exp(math.log(0.03) - 2.3025851 * jax.random.uniform(keys[2], (LAYERS_ALL, ROWS), jnp.float32) ** shard_levels(keys[2], (LAYERS_ALL, ROWS), ((0, 4), (1, 8)), -0.2, 0.2)), 0.003, 0.03),
        "first_columns": jnp.clip(jnp.exp(math.log(0.03) - 2.3025851 * jax.random.uniform(keys[3], (LAYERS_ALL, KV), jnp.float32) ** shard_levels(keys[3], (LAYERS_ALL, KV), ((0, 4),), -0.2, 0.2)), 0.003, 0.03),
        "second_codes": plant(jax.random.randint(keys[4], (LAYERS_ALL, ROWS, KV), 1, 16), jax.random.fold_in(keys[4], 1), 1, 15).astype(jnp.int32),
        "second_rows": jnp.clip(jnp.exp(math.log(0.01) - 2.30258502 * jax.random.uniform(keys[5], (LAYERS_ALL, ROWS), jnp.float32) ** shard_levels(keys[5], (LAYERS_ALL, ROWS), ((0, 4), (1, 8)), -0.2, 0.2)), 0.001, 0.01),
        "second_columns": jnp.clip(jnp.exp(math.log(0.01) - 2.30258502 * jax.random.uniform(keys[6], (LAYERS_ALL, KV), jnp.float32) ** shard_levels(keys[6], (LAYERS_ALL, KV), ((0, 4),), -0.2, 0.2)), 0.001, 0.01),
    }


beta_first = 0.9
beta_second = 0.999
clip_rms = 3.0
epsilon = 1e-08
scale_floor = 0.001

def dequantize(code_values, levels, row_scale, col_scale):
    scale_bound = jnp.minimum(row_scale[:, :, None], col_scale[:, None, :])
    return code_values.astype(jnp.float32) / levels * scale_bound

def moments(gradient, clip_scale, first_codes, first_rows, first_columns, second_codes, second_rows, second_columns):
    first_old = dequantize(first_codes, 7.0, first_rows, first_columns)
    second_old = dequantize(second_codes, 15.0, second_rows, second_columns)
    clipped = clip_scale * gradient
    first_new = beta_first * first_old + (1.0 - beta_first) * clipped
    second_new = beta_second * second_old + (1.0 - beta_second) * clipped * clipped
    direction = first_new / (jnp.sqrt(second_new) + epsilon)
    return (first_new, second_new, direction)

def reference(grad_parts, first_codes, first_rows, first_columns, second_codes, second_rows, second_columns):

    def add_part(which_part, running):
        partial_value = lax.dynamic_index_in_dim(grad_parts, which_part, 1, keepdims=False)
        return running + partial_value.astype(jnp.float32)
    gradient = lax.fori_loop(0, PARTIALS, add_part, jnp.zeros((LAYERS_ALL, ROWS, KV), jnp.float32))
    square_sum = jnp.sum(gradient * gradient)
    clip_limit = clip_rms * math.sqrt(LAYERS_ALL * ROWS * KV)
    clip_scale = clip_limit / jnp.maximum(jnp.sqrt(square_sum), clip_limit)
    first_new, second_new, direction = moments(gradient, clip_scale, first_codes, first_rows, first_columns, second_codes, second_rows, second_columns)
    first_rowmax = jnp.maximum(lax.optimization_barrier(jnp.max(jnp.abs(first_new), axis=2)), scale_floor)
    first_colmax = jnp.maximum(lax.optimization_barrier(jnp.max(jnp.abs(first_new), axis=1)), scale_floor)
    second_rowmax = lax.optimization_barrier(jnp.max(second_new, axis=2))
    second_colmax = lax.optimization_barrier(jnp.max(second_new, axis=1))
    first_scaled = first_new / jnp.minimum(first_rowmax[:, :, None], first_colmax[:, None, :])
    second_scaled = second_new / jnp.minimum(second_rowmax[:, :, None], second_colmax[:, None, :])
    return (direction, first_scaled, second_scaled, first_rowmax, first_colmax, second_rowmax, second_colmax)
```

```python
import functools
import math

import jax
import jax.numpy as jnp
from jax import lax
from jax.experimental import pallas as pl
from jax.experimental.pallas import tpu as pltpu
from jax.sharding import PartitionSpec as P

beta_first = 0.9
beta_second = 0.999
clip_rms = 3.0
epsilon = 1e-08
scale_floor = 0.001

CORES = 2
SLAB = 128
LANES = 128
VMEM_BYTES = 67043328
F32 = jnp.float32


def exchange_kernel(
    chips,
    fsdp,
    sections,
    slabs,
    clip_limit,
    grads,
    first_codes,
    first_rows,
    first_cols,
    second_codes,
    second_rows,
    second_cols,
    first_out,
    second_out,
    first_colmax,
    second_colmax,
    own,
    part,
    right_sum,
    left_sum,
    total,
    codes_a,
    codes_b,
    first,
    second,
    square_send,
    square_recv,
    cross_send,
    cross_recv,
    col_send,
    col_recv,
    own_sem,
    part_send_sem,
    part_recv_sem,
    right_send_sem,
    right_recv_sem,
    left_send_sem,
    left_recv_sem,
    code_sem,
    out_sem,
    square_sems,
    cross_sems,
    col_sems,
):
    me = lax.axis_index("fsdp")
    section = lax.axis_index("section")
    chip = me // CORES
    core = me % CORES
    partner = chip * CORES + (1 - core)
    right = ((chip + 1) % chips) * CORES + core
    left = ((chip + chips - 1) % chips) * CORES + core
    cols = total.shape[-1]
    items = (chips - 1) * slabs

    def own_copy(dest, slab):
        return pltpu.make_async_copy(
            grads.at[dest, core, slab], own.at[dest, slab], own_sem.at[dest * slabs + slab]
        )

    def part_copy(dest, slab):
        return pltpu.make_async_remote_copy(
            src_ref=grads.at[dest, 1 - core, slab],
            dst_ref=part.at[dest, slab],
            send_sem=part_send_sem.at[dest * slabs + slab],
            recv_sem=part_recv_sem.at[dest * slabs + slab],
            device_id={"fsdp": partner},
            device_id_type=pl.DeviceIdType.MESH,
        )

    def right_copy(dest, slab):
        slot = (dest - 1) * slabs + slab
        return pltpu.make_async_remote_copy(
            src_ref=right_sum.at[dest - 1, slab],
            dst_ref=right_sum.at[dest - 1, slab],
            send_sem=right_send_sem.at[slot],
            recv_sem=right_recv_sem.at[slot],
            device_id={"fsdp": right},
            device_id_type=pl.DeviceIdType.MESH,
        )

    def left_copy(dest, slab):
        slot = dest * slabs + slab
        return pltpu.make_async_remote_copy(
            src_ref=left_sum.at[dest, slab],
            dst_ref=left_sum.at[dest, slab],
            send_sem=left_send_sem.at[slot],
            recv_sem=left_recv_sem.at[slot],
            device_id={"fsdp": left},
            device_id_type=pl.DeviceIdType.MESH,
        )

    def wait_pair(dest, slab):
        own_copy(dest, slab).wait()
        part_copy(dest, slab).wait_recv()

    def pair_sum(dest, slab):
        return own[dest, slab].astype(F32) + part[dest, slab].astype(F32)

    @pl.loop(0, chips * slabs)
    def _(i):
        step, slab = i // slabs, i % slabs
        dest = jnp.where(2 * chip < chips, chips - 1 - step, step)
        own_copy(dest, slab).start()
        part_copy(dest, slab).start()

    code_copies = (
        pltpu.make_async_copy(first_codes, codes_a, code_sem.at[0]),
        pltpu.make_async_copy(second_codes, codes_b, code_sem.at[1]),
    )
    for copy in code_copies:
        copy.start()

    @pl.when(chip == 0)
    def _():
        @pl.loop(0, items)
        def _(j):
            dest, slab = chips - 1 - j // slabs, j % slabs
            wait_pair(dest, slab)
            right_sum[dest - 1, slab] = pair_sum(dest, slab)
            right_copy(dest, slab).start()

    @pl.when(chip == chips - 1)
    def _():
        @pl.loop(0, items)
        def _(j):
            dest, slab = j // slabs, j % slabs
            wait_pair(dest, slab)
            left_sum[dest, slab] = pair_sum(dest, slab)
            left_copy(dest, slab).start()

    @pl.loop(0, slabs)
    def _(slab):
        wait_pair(chip, slab)
        total[slab] = pair_sum(chip, slab)

    for copy in code_copies:
        copy.wait()

    @pl.loop(0, slabs)
    def _(slab):
        rows = pl.ds(pl.multiple_of(slab * SLAB, SLAB), SLAB)
        first_row = jnp.broadcast_to(first_rows[:, rows], (LANES, SLAB)).T
        second_row = jnp.broadcast_to(second_rows[:, rows], (LANES, SLAB)).T
        for q in range(cols // LANES):
            span = pl.ds(q * LANES, LANES)
            first_bound = jnp.minimum(first_row, first_cols[:, span])
            second_bound = jnp.minimum(second_row, second_cols[:, span])
            first_old = codes_a[slab, :, span].astype(F32) / 7.0 * first_bound
            second_old = codes_b[slab, :, span].astype(F32) / 15.0 * second_bound
            first[slab, :, span] = beta_first * first_old
            second[slab, :, span] = beta_second * second_old

    @pl.loop(0, items)
    def _(j):
        slab = j % slabs
        dest = chips - 1 - j // slabs

        @pl.when((chip > 0) & (dest > chip))
        def _():
            right_copy(dest, slab).wait_recv()
            wait_pair(dest, slab)
            right_sum[dest - 1, slab] += pair_sum(dest, slab)
            right_copy(dest, slab).start()

        @pl.when((chip > 0) & (dest == chip))
        def _():
            right_copy(dest, slab).wait_recv()
            total[slab] += right_sum[dest - 1, slab]

        low = j // slabs

        @pl.when((chip < chips - 1) & (low < chip))
        def _():
            left_copy(low, slab).wait_recv()
            wait_pair(low, slab)
            left_sum[low, slab] += pair_sum(low, slab)
            left_copy(low, slab).start()

        @pl.when((chip < chips - 1) & (low == chip))
        def _():
            left_copy(low, slab).wait_recv()
            total[slab] += left_sum[low, slab]

    piece = 16
    pieces = SLAB // piece

    def add_squares(i, acc):
        slab, rows = i // pieces, pl.ds(pl.multiple_of((i % pieces) * piece, piece), piece)
        g = total[slab, rows, :]
        return acc + jnp.sum((g * g).reshape(piece // 8, 8, cols), axis=0)

    squares = lax.fori_loop(0, slabs * pieces, add_squares, jnp.zeros((8, cols), F32))
    folded = squares[:, :LANES]
    for q in range(1, cols // LANES):
        folded = folded + squares[:, q * LANES : (q + 1) * LANES]

    def to_all(axis, size, position, source, slots, sems):
        copies = [
            pltpu.make_async_remote_copy(
                src_ref=source,
                dst_ref=slots.at[s - 1],
                send_sem=sems.at[0, s - 1],
                recv_sem=sems.at[1, s - 1],
                device_id={axis: (position + s) % size},
                device_id_type=pl.DeviceIdType.MESH,
            )
            for s in range(1, size)
        ]
        for copy in copies:
            copy.start()
        return copies

    square_send[...] = folded
    square_copies = to_all("fsdp", fsdp, me, square_send, square_recv, square_sems)
    for s, copy in enumerate(square_copies):
        copy.wait_recv()
        folded = folded + square_recv[s]
    cross_send[...] = folded
    cross_copies = to_all("section", sections, section, cross_send, cross_recv, cross_sems)
    for s, copy in enumerate(cross_copies):
        copy.wait_recv()
        folded = folded + cross_recv[s]
    square_sum = jnp.sum(jnp.sum(folded, axis=0, keepdims=True), axis=1, keepdims=True)
    norm = jnp.sqrt(jnp.broadcast_to(square_sum, (1, cols)))
    scale = clip_limit / jnp.maximum(norm, clip_limit)

    def out_copies(slab):
        return (
            pltpu.make_async_copy(first.at[slab], first_out.at[slab], out_sem.at[0, slab]),
            pltpu.make_async_copy(second.at[slab], second_out.at[slab], out_sem.at[1, slab]),
        )

    def update_slab(slab, carry):
        def update_piece(i, carry):
            first_top, second_top = carry
            rows = pl.ds(pl.multiple_of(i * piece, piece), piece)
            clipped = scale * total[slab, rows, :]
            first_new = first[slab, rows, :] + (1.0 - beta_first) * clipped
            second_new = second[slab, rows, :] + (1.0 - beta_second) * clipped * clipped
            first[slab, rows, :] = first_new
            second[slab, rows, :] = second_new
            high = jnp.max(jnp.abs(first_new).reshape(piece // 8, 8, cols), axis=0)
            top = jnp.max(second_new.reshape(piece // 8, 8, cols), axis=0)
            return jnp.maximum(first_top, high), jnp.maximum(second_top, top)

        carry = lax.fori_loop(0, pieces, update_piece, carry)
        for copy in out_copies(slab):
            copy.start()
        return carry

    nothing = jnp.zeros((8, cols), F32)
    first_top, second_top = lax.fori_loop(0, slabs, update_slab, (nothing, nothing))
    first_top = jnp.max(first_top, axis=0, keepdims=True)
    second_top = jnp.max(second_top, axis=0, keepdims=True)
    col_send[0:1, :] = first_top
    col_send[1:2, :] = second_top
    col_copies = to_all("fsdp", fsdp, me, col_send, col_recv, col_sems)

    @pl.loop(0, chips * slabs)
    def _(i):
        part_copy(i // slabs, i % slabs).wait_send()

    @pl.loop(0, items)
    def _(j):
        slab = j % slabs

        @pl.when(j // slabs + 1 > chip)
        def _():
            right_copy(j // slabs + 1, slab).wait_send()

        @pl.when(j // slabs < chip)
        def _():
            left_copy(j // slabs, slab).wait_send()

    for copy in square_copies + cross_copies:
        copy.wait_send()

    for s, copy in enumerate(col_copies):
        copy.wait_recv()
        first_top = jnp.maximum(first_top, col_recv[s, 0:1, :])
        second_top = jnp.maximum(second_top, col_recv[s, 1:2, :])
    first_colmax[...] = jnp.maximum(first_top, scale_floor)
    second_colmax[...] = second_top
    for copy in col_copies:
        copy.wait_send()

    @pl.loop(0, slabs)
    def _(slab):
        for copy in out_copies(slab):
            copy.wait()


def finish_kernel(
    first,
    second,
    first_colmax,
    second_colmax,
    direction,
    first_scaled,
    second_scaled,
    first_rowmax,
    second_rowmax,
):
    first_new = first[0]
    second_new = second[0]
    first_top = jnp.maximum(jnp.max(jnp.abs(first_new), axis=1, keepdims=True), scale_floor)
    second_top = jnp.max(second_new, axis=1, keepdims=True)
    direction[0] = first_new / (jnp.sqrt(second_new) + epsilon)
    first_scaled[0] = first_new / jnp.minimum(first_top, first_colmax[...])
    second_scaled[0] = second_new / jnp.minimum(second_top, second_colmax[...])
    first_rowmax[...] = jnp.broadcast_to(first_top, (SLAB, LANES)).T[0:1, :]
    second_rowmax[...] = jnp.broadcast_to(second_top, (SLAB, LANES)).T[0:1, :]


def local(
    grad_parts, first_codes, first_rows, first_columns, second_codes, second_rows, second_columns
):
    fsdp = lax.axis_size("fsdp")
    sections = lax.axis_size("section")
    layers, _, row_count, cols = grad_parts.shape
    chips = fsdp // CORES
    rows = row_count // fsdp
    slabs = rows // SLAB
    clip_limit = clip_rms * math.sqrt(layers * sections * row_count * cols)
    grads = grad_parts.reshape(chips, CORES, slabs, SLAB, cols)
    tiled = (slabs, SLAB, cols)
    items = (chips - 1) * slabs
    hbm = pl.BlockSpec(memory_space=pl.ANY)
    vmem = pl.BlockSpec(memory_space=pltpu.VMEM)
    dma = pltpu.SemaphoreType.DMA
    first_new, second_new, first_colmax, second_colmax = pl.pallas_call(
        functools.partial(exchange_kernel, chips, fsdp, sections, slabs, clip_limit),
        out_shape=(
            jax.ShapeDtypeStruct(tiled, F32),
            jax.ShapeDtypeStruct(tiled, F32),
            jax.ShapeDtypeStruct((1, cols), F32),
            jax.ShapeDtypeStruct((1, cols), F32),
        ),
        in_specs=[hbm, hbm, vmem, vmem, hbm, vmem, vmem],
        out_specs=(hbm, hbm, vmem, vmem),
        scratch_shapes=[
            pltpu.VMEM((chips, *tiled), jnp.bfloat16),
            pltpu.VMEM((chips, *tiled), jnp.bfloat16),
            pltpu.VMEM((chips - 1, *tiled), F32),
            pltpu.VMEM((chips - 1, *tiled), F32),
            pltpu.VMEM(tiled, F32),
            pltpu.VMEM(tiled, jnp.int32),
            pltpu.VMEM(tiled, jnp.int32),
            pltpu.VMEM(tiled, F32),
            pltpu.VMEM(tiled, F32),
            pltpu.VMEM((8, LANES), F32),
            pltpu.VMEM((fsdp - 1, 8, LANES), F32),
            pltpu.VMEM((8, LANES), F32),
            pltpu.VMEM((max(sections - 1, 1), 8, LANES), F32),
            pltpu.VMEM((2, cols), F32),
            pltpu.VMEM((fsdp - 1, 2, cols), F32),
            dma((chips * slabs,)),
            dma((chips * slabs,)),
            dma((chips * slabs,)),
            dma((items,)),
            dma((items,)),
            dma((items,)),
            dma((items,)),
            dma((2,)),
            dma((2, slabs)),
            dma((2, fsdp - 1)),
            dma((2, max(sections - 1, 1))),
            dma((2, fsdp - 1)),
        ],
        compiler_params=pltpu.CompilerParams(
            has_side_effects=True, vmem_limit_bytes=VMEM_BYTES
        ),
    )(
        grads,
        first_codes.reshape(tiled),
        first_rows,
        first_columns,
        second_codes.reshape(tiled),
        second_rows,
        second_columns,
    )
    block = pl.BlockSpec((1, SLAB, cols), lambda i: (i, 0, 0))
    whole = pl.BlockSpec((1, cols), lambda i: (0, 0))
    strip = pl.BlockSpec((1, SLAB), lambda i: (0, i))
    direction, first_scaled, second_scaled, first_rowmax, second_rowmax = pl.pallas_call(
        finish_kernel,
        grid=(slabs,),
        out_shape=(
            jax.ShapeDtypeStruct(tiled, F32),
            jax.ShapeDtypeStruct(tiled, F32),
            jax.ShapeDtypeStruct(tiled, F32),
            jax.ShapeDtypeStruct((1, rows), F32),
            jax.ShapeDtypeStruct((1, rows), F32),
        ),
        in_specs=[block, block, whole, whole],
        out_specs=(block, block, block, strip, strip),
    )(first_new, second_new, first_colmax, second_colmax)
    shape = (layers, rows, cols)
    return (
        direction.reshape(shape),
        first_scaled.reshape(shape),
        second_scaled.reshape(shape),
        first_rowmax,
        first_colmax,
        second_rowmax,
        second_colmax,
    )


def solution(mesh):
    placed = (
        P("section", "fsdp", None, None),
        P("section", "fsdp", None),
        P("section", "fsdp"),
        P("section", None),
        P("section", "fsdp", None),
        P("section", "fsdp"),
        P("section", None),
    )
    return jax.shard_map(
        local,
        mesh=mesh,
        in_specs=placed,
        out_specs=(
            P("section", "fsdp", None),
            P("section", "fsdp", None),
            P("section", "fsdp", None),
            P("section", "fsdp"),
            P("section", None),
            P("section", "fsdp"),
            P("section", None),
        ),
        check_vma=False,
    )
```

```python
import functools
import math

import jax
import jax.numpy as jnp
from jax import lax
from jax.experimental import pallas as pl
from jax.experimental.pallas import tpu as pltpu
from jax.sharding import PartitionSpec as P

beta_first = 0.9
beta_second = 0.999
clip_rms = 3.0
epsilon = 1e-08
scale_floor = 0.001

CORES = 2
SLAB = 128
LANES = 128
LAG = 2
VMEM_BYTES = 67043328
F32 = jnp.float32


def exchange_kernel(
    chips,
    fsdp,
    sections,
    slabs,
    clip_limit,
    grads,
    first_codes,
    first_rows,
    first_cols,
    second_codes,
    second_rows,
    second_cols,
    first_out,
    second_out,
    first_colmax,
    second_colmax,
    own,
    part,
    right_sum,
    left_sum,
    total,
    codes_a,
    codes_b,
    first,
    second,
    square_send,
    square_recv,
    cross_send,
    cross_recv,
    col_send,
    col_recv,
    own_sem,
    part_send_sem,
    part_recv_sem,
    right_send_sem,
    right_recv_sem,
    left_send_sem,
    left_recv_sem,
    code_sem,
    out_sem,
    square_sems,
    cross_sems,
    col_sems,
):
    me = lax.axis_index("fsdp")
    section = lax.axis_index("section")
    chip = me // CORES
    core = me % CORES
    partner = chip * CORES + (1 - core)
    right = ((chip + 1) % chips) * CORES + core
    left = ((chip + chips - 1) % chips) * CORES + core
    cols = total.shape[-1]
    items = (chips - 1) * slabs

    def own_copy(dest, slab):
        return pltpu.make_async_copy(
            grads.at[dest, core, slab], own.at[dest, slab], own_sem.at[dest * slabs + slab]
        )

    def part_copy(dest, slab):
        return pltpu.make_async_remote_copy(
            src_ref=grads.at[dest, 1 - core, slab],
            dst_ref=part.at[dest, slab],
            send_sem=part_send_sem.at[dest * slabs + slab],
            recv_sem=part_recv_sem.at[dest * slabs + slab],
            device_id={"fsdp": partner},
            device_id_type=pl.DeviceIdType.MESH,
        )

    def right_copy(dest, slab):
        slot = (dest - 1) * slabs + slab
        return pltpu.make_async_remote_copy(
            src_ref=right_sum.at[dest - 1, slab],
            dst_ref=right_sum.at[dest - 1, slab],
            send_sem=right_send_sem.at[slot],
            recv_sem=right_recv_sem.at[slot],
            device_id={"fsdp": right},
            device_id_type=pl.DeviceIdType.MESH,
        )

    def left_copy(dest, slab):
        slot = dest * slabs + slab
        return pltpu.make_async_remote_copy(
            src_ref=left_sum.at[dest, slab],
            dst_ref=left_sum.at[dest, slab],
            send_sem=left_send_sem.at[slot],
            recv_sem=left_recv_sem.at[slot],
            device_id={"fsdp": left},
            device_id_type=pl.DeviceIdType.MESH,
        )

    def wait_pair(dest, slab):
        own_copy(dest, slab).wait()
        part_copy(dest, slab).wait_recv()

    def pair_sum(dest, slab):
        return own[dest, slab].astype(F32) + part[dest, slab].astype(F32)

    @pl.loop(0, chips * slabs)
    def _(i):
        step, slab = i // slabs, i % slabs
        dest = jnp.where(2 * chip < chips, chips - 1 - step, step)
        own_copy(dest, slab).start()
        part_copy(dest, slab).start()

    code_copies = (
        pltpu.make_async_copy(first_codes, codes_a, code_sem.at[0]),
        pltpu.make_async_copy(second_codes, codes_b, code_sem.at[1]),
    )
    for copy in code_copies:
        copy.start()

    @pl.when(chip == 0)
    def _():
        @pl.loop(0, items)
        def _(j):
            dest, slab = chips - 1 - j // slabs, j % slabs
            wait_pair(dest, slab)
            right_sum[dest - 1, slab] = pair_sum(dest, slab)
            right_copy(dest, slab).start()

    @pl.when(chip == chips - 1)
    def _():
        @pl.loop(0, items)
        def _(j):
            dest, slab = j // slabs, j % slabs
            wait_pair(dest, slab)
            left_sum[dest, slab] = pair_sum(dest, slab)
            left_copy(dest, slab).start()

    @pl.loop(0, slabs)
    def _(slab):
        wait_pair(chip, slab)
        total[slab] = pair_sum(chip, slab)

    for copy in code_copies:
        copy.wait()

    @pl.loop(0, slabs)
    def _(slab):
        rows = pl.ds(pl.multiple_of(slab * SLAB, SLAB), SLAB)
        first_row = jnp.broadcast_to(first_rows[:, rows], (LANES, SLAB)).T
        second_row = jnp.broadcast_to(second_rows[:, rows], (LANES, SLAB)).T
        for q in range(cols // LANES):
            span = pl.ds(q * LANES, LANES)
            first_bound = jnp.minimum(first_row, first_cols[:, span])
            second_bound = jnp.minimum(second_row, second_cols[:, span])
            first_old = codes_a[slab, :, span].astype(F32) / 7.0 * first_bound
            second_old = codes_b[slab, :, span].astype(F32) / 15.0 * second_bound
            first[slab, :, span] = beta_first * first_old
            second[slab, :, span] = beta_second * second_old

    right_lag = LAG * chip
    left_lag = LAG * (chips - 1 - chip)

    @pl.loop(0, items + LAG * (chips - 1))
    def _(step):
        j = step - right_lag
        dest = chips - 1 - j // slabs
        slab = j % slabs

        @pl.when((chip > 0) & (j >= 0) & (dest > chip))
        def _():
            right_copy(dest, slab).wait_recv()
            wait_pair(dest, slab)
            right_sum[dest - 1, slab] += pair_sum(dest, slab)
            right_copy(dest, slab).start()

        @pl.when((chip > 0) & (j >= 0) & (dest == chip))
        def _():
            right_copy(dest, slab).wait_recv()
            total[slab] += right_sum[dest - 1, slab]

        i = step - left_lag
        low = i // slabs
        strip = i % slabs

        @pl.when((chip < chips - 1) & (i >= 0) & (low < chip))
        def _():
            left_copy(low, strip).wait_recv()
            wait_pair(low, strip)
            left_sum[low, strip] += pair_sum(low, strip)
            left_copy(low, strip).start()

        @pl.when((chip < chips - 1) & (i >= 0) & (low == chip))
        def _():
            left_copy(low, strip).wait_recv()
            total[strip] += left_sum[low, strip]

    piece = 16
    pieces = SLAB // piece

    def add_squares(i, acc):
        slab, rows = i // pieces, pl.ds(pl.multiple_of((i % pieces) * piece, piece), piece)
        g = total[slab, rows, :]
        return acc + jnp.sum((g * g).reshape(piece // 8, 8, cols), axis=0)

    squares = lax.fori_loop(0, slabs * pieces, add_squares, jnp.zeros((8, cols), F32))
    folded = squares[:, :LANES]
    for q in range(1, cols // LANES):
        folded = folded + squares[:, q * LANES : (q + 1) * LANES]

    def to_all(axis, size, position, source, slots, sems):
        copies = [
            pltpu.make_async_remote_copy(
                src_ref=source,
                dst_ref=slots.at[s - 1],
                send_sem=sems.at[0, s - 1],
                recv_sem=sems.at[1, s - 1],
                device_id={axis: (position + s) % size},
                device_id_type=pl.DeviceIdType.MESH,
            )
            for s in range(1, size)
        ]
        for copy in copies:
            copy.start()
        return copies

    square_send[...] = folded
    square_copies = to_all("fsdp", fsdp, me, square_send, square_recv, square_sems)
    for s, copy in enumerate(square_copies):
        copy.wait_recv()
        folded = folded + square_recv[s]
    cross_send[...] = folded
    cross_copies = to_all("section", sections, section, cross_send, cross_recv, cross_sems)
    for s, copy in enumerate(cross_copies):
        copy.wait_recv()
        folded = folded + cross_recv[s]
    square_sum = jnp.sum(jnp.sum(folded, axis=0, keepdims=True), axis=1, keepdims=True)
    norm = jnp.sqrt(jnp.broadcast_to(square_sum, (1, cols)))
    scale = clip_limit / jnp.maximum(norm, clip_limit)

    def out_copies(slab):
        return (
            pltpu.make_async_copy(first.at[slab], first_out.at[slab], out_sem.at[0, slab]),
            pltpu.make_async_copy(second.at[slab], second_out.at[slab], out_sem.at[1, slab]),
        )

    def update_slab(slab, carry):
        def update_piece(i, carry):
            first_top, second_top = carry
            rows = pl.ds(pl.multiple_of(i * piece, piece), piece)
            clipped = scale * total[slab, rows, :]
            first_new = first[slab, rows, :] + (1.0 - beta_first) * clipped
            second_new = second[slab, rows, :] + (1.0 - beta_second) * clipped * clipped
            first[slab, rows, :] = first_new
            second[slab, rows, :] = second_new
            high = jnp.max(jnp.abs(first_new).reshape(piece // 8, 8, cols), axis=0)
            top = jnp.max(second_new.reshape(piece // 8, 8, cols), axis=0)
            return jnp.maximum(first_top, high), jnp.maximum(second_top, top)

        carry = lax.fori_loop(0, pieces, update_piece, carry)
        for copy in out_copies(slab):
            copy.start()
        return carry

    nothing = jnp.zeros((8, cols), F32)
    first_top, second_top = lax.fori_loop(0, slabs, update_slab, (nothing, nothing))
    first_top = jnp.max(first_top, axis=0, keepdims=True)
    second_top = jnp.max(second_top, axis=0, keepdims=True)
    col_send[0:1, :] = first_top
    col_send[1:2, :] = second_top
    col_copies = to_all("fsdp", fsdp, me, col_send, col_recv, col_sems)

    @pl.loop(0, chips * slabs)
    def _(i):
        part_copy(i // slabs, i % slabs).wait_send()

    @pl.loop(0, items)
    def _(j):
        slab = j % slabs

        @pl.when(j // slabs + 1 > chip)
        def _():
            right_copy(j // slabs + 1, slab).wait_send()

        @pl.when(j // slabs < chip)
        def _():
            left_copy(j // slabs, slab).wait_send()

    for copy in square_copies + cross_copies:
        copy.wait_send()

    for s, copy in enumerate(col_copies):
        copy.wait_recv()
        first_top = jnp.maximum(first_top, col_recv[s, 0:1, :])
        second_top = jnp.maximum(second_top, col_recv[s, 1:2, :])
    first_colmax[...] = jnp.maximum(first_top, scale_floor)
    second_colmax[...] = second_top
    for copy in col_copies:
        copy.wait_send()

    @pl.loop(0, slabs)
    def _(slab):
        for copy in out_copies(slab):
            copy.wait()


def finish_kernel(
    first,
    second,
    first_colmax,
    second_colmax,
    direction,
    first_scaled,
    second_scaled,
    first_rowmax,
    second_rowmax,
    first_kept,
    second_kept,
):
    first_new = first[0]
    second_new = second[0]
    first_top = jnp.maximum(jnp.max(jnp.abs(first_new), axis=1, keepdims=True), scale_floor)
    second_top = jnp.max(second_new, axis=1, keepdims=True)
    direction[0] = first_new / (jnp.sqrt(second_new) + epsilon)
    first_scaled[0] = first_new / jnp.minimum(first_top, first_colmax[...])
    second_scaled[0] = second_new / jnp.minimum(second_top, second_colmax[...])
    first_rowmax[...] = jnp.broadcast_to(first_top, (SLAB, LANES)).T[0:1, :]
    second_rowmax[...] = jnp.broadcast_to(second_top, (SLAB, LANES)).T[0:1, :]
    first_kept[...] = first_colmax[...]
    second_kept[...] = second_colmax[...]


def local(
    grad_parts, first_codes, first_rows, first_columns, second_codes, second_rows, second_columns
):
    fsdp = lax.axis_size("fsdp")
    sections = lax.axis_size("section")
    layers, _, row_count, cols = grad_parts.shape
    chips = fsdp // CORES
    rows = row_count // fsdp
    slabs = rows // SLAB
    clip_limit = clip_rms * math.sqrt(layers * sections * row_count * cols)
    grads = grad_parts.reshape(chips, CORES, slabs, SLAB, cols)
    tiled = (slabs, SLAB, cols)
    items = (chips - 1) * slabs
    hbm = pl.BlockSpec(memory_space=pl.ANY)
    vmem = pl.BlockSpec(memory_space=pltpu.VMEM)
    dma = pltpu.SemaphoreType.DMA
    first_new, second_new, first_colmax, second_colmax = pl.pallas_call(
        functools.partial(exchange_kernel, chips, fsdp, sections, slabs, clip_limit),
        out_shape=(
            jax.ShapeDtypeStruct(tiled, F32),
            jax.ShapeDtypeStruct(tiled, F32),
            jax.ShapeDtypeStruct((1, cols), F32),
            jax.ShapeDtypeStruct((1, cols), F32),
        ),
        in_specs=[hbm, hbm, vmem, vmem, hbm, vmem, vmem],
        out_specs=(hbm, hbm, vmem, vmem),
        scratch_shapes=[
            pltpu.VMEM((chips, *tiled), jnp.bfloat16),
            pltpu.VMEM((chips, *tiled), jnp.bfloat16),
            pltpu.VMEM((chips - 1, *tiled), F32),
            pltpu.VMEM((chips - 1, *tiled), F32),
            pltpu.VMEM(tiled, F32),
            pltpu.VMEM(tiled, jnp.int32),
            pltpu.VMEM(tiled, jnp.int32),
            pltpu.VMEM(tiled, F32),
            pltpu.VMEM(tiled, F32),
            pltpu.VMEM((8, LANES), F32),
            pltpu.VMEM((fsdp - 1, 8, LANES), F32),
            pltpu.VMEM((8, LANES), F32),
            pltpu.VMEM((max(sections - 1, 1), 8, LANES), F32),
            pltpu.VMEM((2, cols), F32),
            pltpu.VMEM((fsdp - 1, 2, cols), F32),
            dma((chips * slabs,)),
            dma((chips * slabs,)),
            dma((chips * slabs,)),
            dma((items,)),
            dma((items,)),
            dma((items,)),
            dma((items,)),
            dma((2,)),
            dma((2, slabs)),
            dma((2, fsdp - 1)),
            dma((2, max(sections - 1, 1))),
            dma((2, fsdp - 1)),
        ],
        compiler_params=pltpu.CompilerParams(
            has_side_effects=True, vmem_limit_bytes=VMEM_BYTES
        ),
    )(
        grads,
        first_codes.reshape(tiled),
        first_rows,
        first_columns,
        second_codes.reshape(tiled),
        second_rows,
        second_columns,
    )
    block = pl.BlockSpec((1, SLAB, cols), lambda i: (i, 0, 0))
    whole = pl.BlockSpec((1, cols), lambda i: (0, 0))
    strip = pl.BlockSpec((1, SLAB), lambda i: (0, i))
    finished = pl.pallas_call(
        finish_kernel,
        grid=(slabs,),
        out_shape=(
            jax.ShapeDtypeStruct(tiled, F32),
            jax.ShapeDtypeStruct(tiled, F32),
            jax.ShapeDtypeStruct(tiled, F32),
            jax.ShapeDtypeStruct((1, rows), F32),
            jax.ShapeDtypeStruct((1, rows), F32),
            jax.ShapeDtypeStruct((1, cols), F32),
            jax.ShapeDtypeStruct((1, cols), F32),
        ),
        in_specs=[block, block, whole, whole],
        out_specs=(block, block, block, strip, strip, whole, whole),
    )(first_new, second_new, first_colmax, second_colmax)
    direction, first_scaled, second_scaled = finished[:3]
    first_rowmax, second_rowmax, first_colmax, second_colmax = finished[3:]
    shape = (layers, rows, cols)
    return (
        direction.reshape(shape),
        first_scaled.reshape(shape),
        second_scaled.reshape(shape),
        first_rowmax,
        first_colmax,
        second_rowmax,
        second_colmax,
    )


def solution(mesh):
    placed = (
        P("section", "fsdp", None, None),
        P("section", "fsdp", None),
        P("section", "fsdp"),
        P("section", None),
        P("section", "fsdp", None),
        P("section", "fsdp"),
        P("section", None),
    )
    return jax.shard_map(
        local,
        mesh=mesh,
        in_specs=placed,
        out_specs=(
            P("section", "fsdp", None),
            P("section", "fsdp", None),
            P("section", "fsdp", None),
            P("section", "fsdp"),
            P("section", None),
            P("section", "fsdp"),
            P("section", None),
        ),
        check_vma=False,
    )
```
